32 devices in a mesh: dp: 2 (over x), ep: 16 (over y, z, core).
Axes of the slice: x: 2, y: 2, z: 4, core: 2. Of those that a mesh axis runs over, the one named last changes fastest.
Arguments:
- x: bfloat16 [2, 16, 256, 3072], P('dp', 'ep'), parts along dimension 0
- expert: int32 [2, 16, 256, 4], P('dp', 'ep'), parts along dimension 0
- slot: int32 [2, 16, 256, 4], P('dp', 'ep'), parts along dimension 0
- gate: float32 [2, 16, 256, 4], P('dp', 'ep'), parts along dimension 0
- w_gate: bfloat16 [16, 3072, 10752], P('ep')
- w_up: bfloat16 [16, 3072, 10752], P('ep')
- w_down: bfloat16 [16, 10752, 3072], P('ep')
Outputs:
- y: bfloat16 [2, 16, 256, 3072], P('dp', 'ep'), parts along dimension 0
There are 2 independent parts. The reference program is written for one: setup_inputs(seed, part) draws one part's arguments, and reference() takes and returns one part's arrays. A program takes and returns all parts, laid end to end along the dimension named above; an argument that names none is the same for every part.
All inputs are finite; a program needn't handle non-finite values.
Results may differ from the reference program's by a relative error of at most 0.009.
Values are sent between devices in bfloat16 or wider.
A program may use at most 2 GiB of HBM per device.

```python
import jax
import jax.numpy as jnp

MEMBERS = 16
TOKENS = 256
D = 3072
FF = 10752
TOP = 4
EXPERTS = 16
SLOTS = 5 * TOKENS * TOP // (4 * EXPERTS)


def setup_inputs(seed: int = 0, part: int = 0) -> dict:
    own, k1, k2, k3, k4, k5, k6 = jax.random.split(jax.random.key(seed), 7)
    kx, ke, kl, kg = jax.random.split(jax.random.fold_in(own, part), 4)
    devices = (1, MEMBERS)
    place = jax.random.permutation(kl, jnp.arange(EXPERTS, dtype=jnp.uint32))
    slow = ((EXPERTS + (9 * place) % EXPERTS) << ((9 * place) // EXPERTS)) // EXPERTS
    wait = (jax.random.bits(ke, (*devices, TOKENS, EXPERTS), jnp.uint32) >> 10) * slow
    expert = jnp.argsort(wait, axis=-1)[..., :TOP].astype(jnp.int32)
    chosen = jax.nn.one_hot(expert, EXPERTS, dtype=jnp.int32)
    in_line = jnp.cumsum(chosen.reshape(*devices, TOKENS * TOP, EXPERTS), axis=2) - 1
    slot = jnp.sum(in_line.reshape(chosen.shape) * chosen, axis=-1)

    def one(key, rows, columns):
        return (jax.random.normal(key, (rows, columns), jnp.float32) * rows**-0.5).astype(jnp.bfloat16)

    def weights(key, rows, columns):
        return jax.lax.map(lambda k: one(k, rows, columns), jax.random.split(key, EXPERTS))

    return {
        "x": jax.random.normal(kx, (*devices, TOKENS, D), jnp.float32).astype(jnp.bfloat16),
        "expert": expert,
        "slot": slot,
        "gate": jax.nn.softmax(jax.random.normal(kg, expert.shape, jnp.float32)),
        "w_gate": weights(k1, D, FF),
        "w_up": weights(k2, D, FF),
        "w_down": weights(k3, FF, D),
    }


def einsum(form, a, b):
    return jnp.einsum(form, a.astype(jnp.float32), b.astype(jnp.float32))


def reference(x, expert, slot, gate, w_gate, w_up, w_down):
    to_expert = jax.nn.one_hot(expert, EXPERTS, dtype=jnp.bfloat16)
    to_slot = jax.nn.one_hot(slot, SLOTS, dtype=jnp.bfloat16)
    weighted = to_expert * gate[..., None].astype(jnp.bfloat16)
    dispatch = einsum("abtke,abtkc->abtec", to_expert, to_slot).astype(jnp.bfloat16)
    combine = einsum("abtke,abtkc->abtec", weighted, to_slot).astype(jnp.bfloat16)
    z = einsum("abtec,abtd->aebcd", dispatch, x).astype(jnp.bfloat16)
    h = jax.nn.silu(einsum("aebcd,edf->aebcf", z, w_gate))
    h = (h * einsum("aebcd,edf->aebcf", z, w_up)).astype(jnp.bfloat16)
    out = einsum("aebcf,efd->aebcd", h, w_down).astype(jnp.bfloat16)
    y = einsum("abtec,aebcd->abtd", combine, out)
    return y.astype(jnp.bfloat16)
```

```python
import functools

import jax
import jax.numpy as jnp
from jax import lax
from jax.experimental import pallas as pl
from jax.experimental.pallas import tpu as pltpu
from jax.sharding import PartitionSpec as P

MESH = pl.DeviceIdType.MESH
F32, BF16 = jnp.float32, jnp.bfloat16
SLOTS, TOK, D, FF = 80, 256, 3072, 10752
LAYER = 4 * SLOTS
VMEM_LIMIT = 67043328
PEERS = ((0, 1), (1, 0), (1, 1))


def place():
    e = lax.axis_index("ep")
    return e // 8, (e // 2) % 4, e % 2


def flip(v, d):
    return 1 - v if d else v


def ep_of(y, z, c):
    return y * 8 + z * 2 + c


def neighbours(z):
    return 3 + (z + 2) // 3 + (5 - z) // 3


def layer_order(z, k):
    half = z // 2
    zz = z + half * (3 - 2 * z)
    far = k // 2
    low = far * k + (1 - far) * (zz + k - 2 * zz * k)
    return low + half * (3 - 2 * low)


def slot_rows(expert, info):
    rows = (lax.broadcasted_iota(jnp.int32, (SLOTS, TOK), 0) + expert * SLOTS).astype(F32)
    return [rows == info[j : j + 1, :] for j in range(4)]


TN = 512
NT = FF // TN
NB = 3
KSPLIT = 2
EVENT, GAP = 7, 17


def up_kernel(info_ref, x_ref, wg_hbm, wu_hbm, h_hbm, info_out,
              xbuf, zbuf, stage, ibuf, wbuf, hbuf,
              wsem, hsem, ssem, rsem, xsend, xrecv, isend, irecv):
    y, z, c = place()
    q = y * 2 + c
    inward = 1 - 2 * (z // 2)
    barrier = pltpu.get_barrier_semaphore()

    def at(zz):
        return {"ep": ep_of(y, zz, c)}

    def peer(r):
        dy, dc = PEERS[r]
        return flip(y, dy), flip(c, dc)

    for r in range(3):
        yy, cc = peer(r)
        pl.semaphore_signal(barrier, inc=1, device_id={"ep": ep_of(yy, z, cc)}, device_id_type=MESH)

    @pl.when(z > 0)
    def _():
        pl.semaphore_signal(barrier, inc=1, device_id=at(z - 1), device_id_type=MESH)

    @pl.when(z < 3)
    def _():
        pl.semaphore_signal(barrier, inc=1, device_id=at(z + 1), device_id_type=MESH)

    def weights(g, start):
        t = lax.rem(g, NT)
        b = lax.rem(g, NB)
        depth = D // KSPLIT
        for m, hbm in enumerate((wg_hbm, wu_hbm)):
            for r in range(KSPLIT):
                copy = pltpu.make_async_copy(
                    hbm.at[pl.ds(r * depth, depth), pl.ds(pl.multiple_of(t * TN, TN), TN)],
                    wbuf.at[b, m, pl.ds(r * depth, depth), :],
                    wsem.at[b, m, r],
                )
                if start:
                    copy.start()
                else:
                    copy.wait()

    for g in range(NB - 1):
        weights(g, True)

    def along(src_x, src_i, slot, to, way):
        return tuple(
            pltpu.make_async_remote_copy(
                src_ref=src,
                dst_ref=dst.at[slot],
                send_sem=send.at[way, slot],
                recv_sem=recv.at[slot],
                device_id=at(to),
                device_id_type=MESH,
            )
            for src, dst, send, recv in ((src_i, ibuf, isend, irecv), (src_x, xbuf, xsend, xrecv))
        )

    def swap(slot, r):
        yy, cc = peer(r)
        return pltpu.make_async_remote_copy(
            src_ref=stage.at[slot, r],
            dst_ref=zbuf.at[slot * 4 + q],
            send_sem=ssem.at[slot, r],
            recv_sem=rsem.at[slot * 4 + q],
            device_id={"ep": ep_of(yy, z, cc)},
            device_id_type=MESH,
        )

    def swap_in(slot, r):
        yy, cc = peer(r)
        return pltpu.make_async_remote_copy(
            src_ref=stage.at[slot, r],
            dst_ref=zbuf.at[slot * 4 + yy * 2 + cc],
            send_sem=ssem.at[slot, r],
            recv_sem=rsem.at[slot * 4 + yy * 2 + cc],
            device_id={"ep": ep_of(yy, z, cc)},
            device_id_type=MESH,
        )

    def deal(slot, info, x):
        def gathered(yy, cc):
            hit = slot_rows(ep_of(yy, z, cc), info)
            pick = (hit[0] | hit[1] | hit[2] | hit[3]).astype(F32).astype(BF16)
            return jnp.dot(pick, x, preferred_element_type=F32).astype(BF16)

        for n, r in enumerate((1, 2, 0)):
            stage[slot, r] = gathered(*peer(r))
            if n:
                swap(slot, (1, 2, 0)[n - 1]).start()
        zbuf[slot * 4 + q] = gathered(y, c)
        swap(slot, 0).start()

    pl.semaphore_wait(barrier, neighbours(z))

    @pl.when(z < 3)
    def _():
        for copy in along(x_ref, info_ref, z, z + 1, 1):
            copy.start()

    @pl.when(z > 0)
    def _():
        for copy in along(x_ref, info_ref, z, z - 1, 0):
            copy.start()

    deal(z, info_ref[...], x_ref[...])

    def receive(hops):
        def side(n, deal_out):
            way = inward * (1 - 2 * n)
            slot = z - way * hops
            to = z + way
            here = (slot >= 0) & (slot < 4)

            @pl.when(here)
            def _():
                if deal_out:
                    deal(slot, ibuf[slot], xbuf[slot])
                else:
                    for copy in along(xbuf.at[slot], ibuf.at[slot], slot, z, 0):
                        copy.wait_recv()

                    @pl.when((to >= 0) & (to < 4))
                    def _():
                        for copy in along(xbuf.at[slot], ibuf.at[slot], slot, to, (way + 1) // 2):
                            copy.start()

        for deal_out in (False, True):
            def both(n, carry, deal_out=deal_out):
                side(n, deal_out)
                return carry

            lax.fori_loop(0, 2, both, 0)

    def put(g):
        k = g // NT
        t = lax.rem(g, NT)
        zl = layer_order(z, k)
        b = lax.rem(g, 2)
        return pltpu.make_async_copy(
            hbuf.at[b],
            h_hbm.at[pl.ds(pl.multiple_of(zl * LAYER, LAYER), LAYER), pl.ds(pl.multiple_of(t * TN, TN), TN)],
            hsem.at[b],
        )

    def body(g, carry):
        k = g // NT
        t = lax.rem(g, NT)
        zl = layer_order(z, k)

        @pl.when((g >= EVENT) & (lax.rem(g + GAP - EVENT, GAP) == 0) & (g <= EVENT + 2 * GAP))
        def _():
            receive((g - EVENT) // GAP + 1)

        @pl.when(t == 0)
        def _():
            for r in range(3):
                swap_in(zl, r).wait_recv()

        weights(g, False)

        @pl.when(g + NB - 1 < 4 * NT)
        def _():
            weights(g + NB - 1, True)

        @pl.when(g >= 2)
        def _():
            put(g - 2).wait()

        b = lax.rem(g, NB)
        o = lax.rem(g, 2)
        rows = zbuf[pl.ds(zl * 4, 4)].reshape(LAYER, D)
        for r in range(TN // 256):
            cols = slice(r * 256, (r + 1) * 256)
            gate = jnp.dot(rows, wbuf[b, 0, :, cols], preferred_element_type=F32)
            up = jnp.dot(rows, wbuf[b, 1, :, cols], preferred_element_type=F32)
            hbuf[o, :, cols] = (jax.nn.silu(gate) * up).astype(BF16)
        put(g).start()
        return carry

    lax.fori_loop(0, 4 * NT, body, 0)
    put(4 * NT - 2).wait()
    put(4 * NT - 1).wait()
    for slot in range(4):
        for r in range(3):
            swap(slot, r).wait_send()

        @pl.when((z >= slot) & (z < 3))
        def _():
            for copy in along(x_ref, info_ref, slot, z, 1):
                copy.wait_send()

        @pl.when((z <= slot) & (z > 0))
        def _():
            for copy in along(x_ref, info_ref, slot, z, 0):
                copy.wait_send()

        @pl.when(z != slot)
        def _():
            info_out[slot] = ibuf[slot]

        @pl.when(z == slot)
        def _():
            info_out[slot] = info_ref[...]


W = 256
NS = D // W
LAG = 2


def down_kernel(info_ref, h_hbm, wd_hbm, y_ref,
                hv, wbuf, obuf, rbuf, stage, ubuf, comb,
                hsem, wsem, osend, orecv, usend, urecv):
    y, z, c = place()
    q = y * 2 + c
    barrier = pltpu.get_barrier_semaphore()

    def at(zz):
        return {"ep": ep_of(y, zz, c)}

    for dy, dc in PEERS:
        pl.semaphore_signal(barrier, inc=1, device_id={"ep": ep_of(flip(y, dy), z, flip(c, dc))}, device_id_type=MESH)

    @pl.when(z > 0)
    def _():
        pl.semaphore_signal(barrier, inc=1, device_id=at(z - 1), device_id_type=MESH)

    @pl.when(z < 3)
    def _():
        pl.semaphore_signal(barrier, inc=1, device_id=at(z + 1), device_id_type=MESH)

    def weights(s):
        b = lax.rem(s, 2)
        return pltpu.make_async_copy(
            wd_hbm.at[:, pl.ds(pl.multiple_of(s * W, W), W)], wbuf.at[b], wsem.at[b]
        )

    def h_rows(n):
        rows = pl.ds(pl.multiple_of(n * LAYER, LAYER), LAYER)
        return pltpu.make_async_copy(h_hbm.at[rows], hv.at[rows], hsem.at[n])

    weights(0).start()
    for n in range(4):
        h_rows(n).start()
    for d in range(4):
        info = info_ref[d]
        for e in range(4):
            hit = slot_rows(ep_of(e // 2, z, e % 2), info)
            total = jnp.where(hit[0], info[4:5, :], 0.0)
            for j in range(1, 4):
                total += jnp.where(hit[j], info[4 + j : 5 + j, :], 0.0)
            comb[d, e * SLOTS : (e + 1) * SLOTS, :] = total.astype(BF16)
    pl.semaphore_wait(barrier, neighbours(z))

    def across(s, r):
        dy, dc = PEERS[r]
        yy, cc = flip(y, dy), flip(c, dc)
        return pltpu.make_async_remote_copy(
            src_ref=obuf.at[lax.rem(s, 2), yy * 2 + cc],
            dst_ref=rbuf.at[s, :, q],
            send_sem=osend.at[lax.rem(s, 2), r],
            recv_sem=orecv.at[s, q],
            device_id={"ep": ep_of(yy, z, cc)},
            device_id_type=MESH,
        )

    def across_in(s, r):
        dy, dc = PEERS[r]
        yy, cc = flip(y, dy), flip(c, dc)
        return pltpu.make_async_remote_copy(
            src_ref=obuf.at[0, 0],
            dst_ref=rbuf.at[s, :, yy * 2 + cc],
            send_sem=osend.at[0, r],
            recv_sem=orecv.at[s, yy * 2 + cc],
            device_id={"ep": ep_of(yy, z, cc)},
            device_id_type=MESH,
        )

    def hop(s, d, to, slot):
        return pltpu.make_async_remote_copy(
            src_ref=stage.at[lax.rem(s, 2), d],
            dst_ref=ubuf.at[s, slot],
            send_sem=usend.at[lax.rem(s, 2), d],
            recv_sem=urecv.at[s, slot],
            device_id=at(to),
            device_id_type=MESH,
        )

    def part(s, d):
        rows = rbuf[s, d].reshape(LAYER, W)
        return lax.dot_general(comb[d], rows, (((0,), (0,)), ((), ())), preferred_element_type=F32)

    def live(s):
        return (s >= 0) & (s < NS)

    def towards(i, d, up):
        s = i - LAG - (z if up else 3 - z)

        @pl.when(live(s) & ((z < d) if up else (z > d)))
        def _():
            total = part(s, d)

            @pl.when(s >= 2)
            def _():
                hop(s - 2, d, z, d).wait_send()

            @pl.when(z == (0 if up else 3))
            def _():
                stage[lax.rem(s, 2), d] = total.astype(BF16)

            @pl.when(z != (0 if up else 3))
            def _():
                hop(s, d, z, d).wait_recv()
                stage[lax.rem(s, 2), d] = (total + ubuf[s, d].astype(F32)).astype(BF16)

    def launch(i, d, up):
        s = i - LAG - (z if up else 3 - z)
        if up:
            @pl.when(live(s) & (z < d))
            def _():
                hop(s, d, z + 1, d).start()
        else:
            @pl.when(live(s) & (z > d + 1))
            def _():
                hop(s, d, z - 1, d).start()

            @pl.when(live(s) & (z == d + 1))
            def _():
                hop(s, d, z - 1, 4).start()

    def finish(i, d):
        s = i - LAG - max(d, 3 - d)

        @pl.when(live(s) & (z == d))
        def _():
            total = part(s, d)
            if d > 0:
                hop(s, d, z, d).wait_recv()
                total += ubuf[s, d].astype(F32)
            if d < 3:
                hop(s, d, z, 4).wait_recv()
                total += ubuf[s, 4].astype(F32)
            y_ref[:, pl.ds(pl.multiple_of(s * W, W), W)] = total.astype(BF16)

    def body(i, carry):
        @pl.when((i >= LAG) & (i < NS + LAG))
        def _():
            for r in range(3):
                across_in(i - LAG, r).wait_recv()

        steps = [(3, True), (0, False), (2, True), (1, False), (1, True), (2, False)]
        for d, up in steps:
            towards(i, d, up)
        for d, up in steps:
            launch(i, d, up)
        for d in range(4):
            finish(i, d)

        @pl.when(i < NS)
        def _():
            b = lax.rem(i, 2)
            weights(i).wait()

            @pl.when(i + 1 < NS)
            def _():
                weights(i + 1).start()

            @pl.when(i >= 2)
            def _():
                for r in range(3):
                    across(i - 2, r).wait_send()

            def rows(n, carry):
                @pl.when(i == 0)
                def _():
                    h_rows(2 * n).wait()
                    h_rows(2 * n + 1).wait()

                out = jnp.dot(
                    hv[pl.ds(pl.multiple_of(n * 2 * LAYER, LAYER), 2 * LAYER), :], wbuf[b], preferred_element_type=F32
                ).astype(BF16)
                for m in range(8):
                    obuf[b, m % 4, 2 * n + m // 4] = out[m * SLOTS : (m + 1) * SLOTS, :]
                return carry

            lax.fori_loop(0, 2, rows, 0)
            rbuf[i, :, q] = obuf[b, q]
            for r in (1, 2, 0):
                across(i, r).start()

        return carry

    lax.fori_loop(0, NS + LAG + 3, body, 0)
    for s in (NS - 2, NS - 1):
        for r in range(3):
            across(s, r).wait_send()
        for d in range(4):
            @pl.when(z != d)
            def _():
                hop(s, d, z, d).wait_send()


def any_space():
    return pl.BlockSpec(memory_space=pl.ANY)


def vmem():
    return pl.BlockSpec(memory_space=pltpu.VMEM)


def project_up(info, x, wg, wu):
    rows = 16 * SLOTS
    return pl.pallas_call(
        up_kernel,
        out_shape=(jax.ShapeDtypeStruct((rows, FF), BF16), jax.ShapeDtypeStruct((4, 8, TOK), F32)),
        in_specs=[vmem(), vmem(), any_space(), any_space()],
        out_specs=(any_space(), vmem()),
        scratch_shapes=[
            pltpu.VMEM((4, TOK, D), BF16),
            pltpu.VMEM((16, SLOTS, D), BF16),
            pltpu.VMEM((4, 3, SLOTS, D), BF16),
            pltpu.VMEM((4, 8, TOK), F32),
            pltpu.VMEM((NB, 2, D, TN), BF16),
            pltpu.VMEM((2, LAYER, TN), BF16),
            pltpu.SemaphoreType.DMA((NB, 2, KSPLIT)),
            pltpu.SemaphoreType.DMA((2,)),
            pltpu.SemaphoreType.DMA((4, 3)),
            pltpu.SemaphoreType.DMA((16,)),
            pltpu.SemaphoreType.DMA((2, 4)),
            pltpu.SemaphoreType.DMA((4,)),
            pltpu.SemaphoreType.DMA((2, 4)),
            pltpu.SemaphoreType.DMA((4,)),
        ],
        compiler_params=pltpu.CompilerParams(
            collective_id=0, has_side_effects=True, vmem_limit_bytes=VMEM_LIMIT
        ),
        cost_estimate=pl.CostEstimate(
            flops=4 * rows * D * FF, bytes_accessed=16 * D * FF + 2 * rows * FF, transcendentals=rows * FF
        ),
        name="project_up",
    )(info, x, wg, wu)


def project_down(info, h, wd):
    rows = 16 * SLOTS
    return pl.pallas_call(
        down_kernel,
        out_shape=jax.ShapeDtypeStruct((TOK, D), BF16),
        in_specs=[vmem(), any_space(), any_space()],
        out_specs=vmem(),
        scratch_shapes=[
            pltpu.VMEM((rows, FF), BF16),
            pltpu.VMEM((2, FF, W), BF16),
            pltpu.VMEM((2, 4, 4, SLOTS, W), BF16),
            pltpu.VMEM((NS, 4, 4, SLOTS, W), BF16),
            pltpu.VMEM((2, 4, TOK, W), BF16),
            pltpu.VMEM((NS, 5, TOK, W), BF16),
            pltpu.VMEM((4, LAYER, TOK), BF16),
            pltpu.SemaphoreType.DMA((4,)),
            pltpu.SemaphoreType.DMA((2,)),
            pltpu.SemaphoreType.DMA((2, 3)),
            pltpu.SemaphoreType.DMA((NS, 4)),
            pltpu.SemaphoreType.DMA((2, 4)),
            pltpu.SemaphoreType.DMA((NS, 5)),
        ],
        compiler_params=pltpu.CompilerParams(
            collective_id=1, has_side_effects=True, vmem_limit_bytes=VMEM_LIMIT
        ),
        cost_estimate=pl.CostEstimate(
            flops=2 * rows * D * FF, bytes_accessed=2 * D * FF + 2 * rows * FF, transcendentals=0
        ),
        name="project_down",
    )(info, h, wd)


def solution(mesh):
    def step(x, expert, slot, gate, wg, wu, wd):
        where = jnp.where(slot[0, 0] < SLOTS, expert[0, 0] * SLOTS + slot[0, 0], -1).astype(F32)
        info = jnp.concatenate([where.T, gate[0, 0].T], axis=0)
        h, infos = project_up(info, x[0, 0], wg[0], wu[0])
        return project_down(infos, h, wd[0])[None, None]

    tokens = P("dp", "ep")
    experts = P("ep")
    return jax.shard_map(
        step,
        mesh=mesh,
        in_specs=(tokens, tokens, tokens, tokens, experts, experts, experts),
        out_specs=tokens,
        check_vma=False,
    )
```

```python
import functools

import jax
import jax.numpy as jnp
from jax import lax
from jax.experimental import pallas as pl
from jax.experimental.pallas import tpu as pltpu
from jax.sharding import PartitionSpec as P

MESH = pl.DeviceIdType.MESH
F32, BF16 = jnp.float32, jnp.bfloat16
SLOTS, TOK, D, FF = 80, 256, 3072, 10752
LAYER = 4 * SLOTS
VMEM_LIMIT = 67043328
PEERS = ((0, 1), (1, 0), (1, 1))


def place():
    e = lax.axis_index("ep")
    return e // 8, (e // 2) % 4, e % 2


def flip(v, d):
    return 1 - v if d else v


def ep_of(y, z, c):
    return y * 8 + z * 2 + c


def neighbours(z):
    return 3 + (z + 2) // 3 + (5 - z) // 3


def layer_order(z, k):
    half = z // 2
    zz = z + half * (3 - 2 * z)
    far = k // 2
    low = far * k + (1 - far) * (zz + k - 2 * zz * k)
    return low + half * (3 - 2 * low)


def slot_rows(expert, info):
    rows = (lax.broadcasted_iota(jnp.int32, (SLOTS, TOK), 0) + expert * SLOTS).astype(F32)
    return [rows == info[j : j + 1, :] for j in range(4)]


TN = 512
NT = FF // TN
NB = 4
KSPLIT = 2
HEAD = 10
DEAL = 512
EVENT, GAP = 18, 16


def up_kernel(info_ref, x_ref, wg_hbm, wu_hbm, h_hbm, info_out,
              xbuf, zbuf, stage, ibuf, wbuf, hbuf,
              wsem, hsem, ssem, rsem, xsend, xrecv, isend, irecv):
    y, z, c = place()
    q = y * 2 + c
    inward = 1 - 2 * (z // 2)
    barrier = pltpu.get_barrier_semaphore()

    def at(zz):
        return {"ep": ep_of(y, zz, c)}

    def peer(r):
        dy, dc = PEERS[r]
        return flip(y, dy), flip(c, dc)

    for r in range(3):
        yy, cc = peer(r)
        pl.semaphore_signal(barrier, inc=1, device_id={"ep": ep_of(yy, z, cc)}, device_id_type=MESH)

    @pl.when(z > 0)
    def _():
        pl.semaphore_signal(barrier, inc=1, device_id=at(z - 1), device_id_type=MESH)

    @pl.when(z < 3)
    def _():
        pl.semaphore_signal(barrier, inc=1, device_id=at(z + 1), device_id_type=MESH)

    def weights(g, start):
        t = lax.rem(g, NT)
        b = lax.rem(g, NB)
        depth = D // KSPLIT
        for m, hbm in enumerate((wg_hbm, wu_hbm)):
            for r in range(KSPLIT):
                copy = pltpu.make_async_copy(
                    hbm.at[pl.ds(r * depth, depth), pl.ds(pl.multiple_of(t * TN, TN), TN)],
                    wbuf.at[b, m, pl.ds(r * depth, depth), :],
                    wsem.at[b, m, r],
                )
                if start:
                    copy.start()
                else:
                    copy.wait()

    for g in range(NB - 1):
        weights(g, True)

    def along(src_x, src_i, slot, to, way):
        return tuple(
            pltpu.make_async_remote_copy(
                src_ref=src,
                dst_ref=dst.at[slot],
                send_sem=send.at[way, slot],
                recv_sem=recv.at[slot],
                device_id=at(to),
                device_id_type=MESH,
            )
            for src, dst, send, recv in ((src_i, ibuf, isend, irecv), (src_x, xbuf, xsend, xrecv))
        )

    def swap(slot, r):
        yy, cc = peer(r)
        return pltpu.make_async_remote_copy(
            src_ref=stage.at[slot, r],
            dst_ref=zbuf.at[slot * 4 + q],
            send_sem=ssem.at[slot, r],
            recv_sem=rsem.at[slot * 4 + q],
            device_id={"ep": ep_of(yy, z, cc)},
            device_id_type=MESH,
        )

    def swap_in(slot, r):
        yy, cc = peer(r)
        return pltpu.make_async_remote_copy(
            src_ref=stage.at[slot, r],
            dst_ref=zbuf.at[slot * 4 + yy * 2 + cc],
            send_sem=ssem.at[slot, r],
            recv_sem=rsem.at[slot * 4 + yy * 2 + cc],
            device_id={"ep": ep_of(yy, z, cc)},
            device_id_type=MESH,
        )

    def deal(slot, info, x):
        def pick(yy, cc):
            hit = slot_rows(ep_of(yy, z, cc), info)
            return (hit[0] | hit[1] | hit[2] | hit[3]).astype(F32).astype(BF16)

        picks = jnp.concatenate([pick(*peer(r)) for r in (1, 2, 0)] + [pick(y, c)], axis=0)
        for n in range(D // DEAL):
            cols = slice(n * DEAL, (n + 1) * DEAL)
            rows = jnp.dot(picks, x[:, cols], preferred_element_type=F32).astype(BF16)
            for m, r in enumerate((1, 2, 0)):
                stage[slot, r, :, cols] = rows[m * SLOTS : (m + 1) * SLOTS, :]
            zbuf[slot * 4 + q, :, cols] = rows[3 * SLOTS :, :]
        for r in (1, 2, 0):
            swap(slot, r).start()

    pl.semaphore_wait(barrier, neighbours(z))

    @pl.when(z < 3)
    def _():
        for copy in along(x_ref, info_ref, z, z + 1, 1):
            copy.start()

    @pl.when(z > 0)
    def _():
        for copy in along(x_ref, info_ref, z, z - 1, 0):
            copy.start()

    deal(z, info_ref[...], x_ref)

    def receive(hops):
        def side(n, deal_out):
            way = inward * (1 - 2 * n)
            slot = z - way * hops
            to = z + way
            here = (slot >= 0) & (slot < 4)

            @pl.when(here)
            def _():
                if deal_out:
                    deal(slot, ibuf[slot], xbuf.at[slot])
                else:
                    for copy in along(xbuf.at[slot], ibuf.at[slot], slot, z, 0):
                        copy.wait_recv()

                    @pl.when((to >= 0) & (to < 4))
                    def _():
                        for copy in along(xbuf.at[slot], ibuf.at[slot], slot, to, (way + 1) // 2):
                            copy.start()

        for deal_out in (False, True):
            def both(n, carry, deal_out=deal_out):
                side(n, deal_out)
                return carry

            lax.fori_loop(0, 2, both, 0)

    def plan(g):
        k = g // NT
        t = lax.rem(g, NT)
        zl = layer_order(z, k)
        head = (NT - 1 - t) // (NT - HEAD)
        start = (3 - k) // 3
        before = layer_order(z, k - 1 + start)
        other = zl + head * (1 - start) * (before - zl)
        pieces = (
            other * 4 + (1 - y) * 2,
            zl * 4 + y * 2,
            zl * 4 + (start * y + (1 - start) * (1 - y)) * 2,
        )
        pair = (k > 0) | (t >= HEAD)
        lone = ((k == 0) | (k == 3)) & (t < HEAD)
        return k, t, zl, pieces, pair, lone

    def put(g, wait):
        k, t, zl, pieces, pair, lone = plan(g)
        b = lax.rem(g, 2)
        copies = [
            pltpu.make_async_copy(
                hbuf.at[b, n],
                h_hbm.at[
                    pl.ds(pl.multiple_of(pieces[n] * SLOTS, 2 * SLOTS), 2 * SLOTS),
                    pl.ds(pl.multiple_of(t * TN, TN), TN),
                ],
                hsem.at[b, n],
            )
            for n in range(3)
        ]

        def each(chosen):
            for copy in chosen:
                if wait:
                    copy.wait()
                else:
                    copy.start()

        @pl.when(pair)
        def _():
            each(copies[:2])

        @pl.when(lone)
        def _():
            each(copies[2:])

    def body(g, carry):
        k, t, zl, pieces, pair, lone = plan(g)

        @pl.when((g >= EVENT) & (lax.rem(g + GAP - EVENT, GAP) == 0) & (g <= EVENT + 2 * GAP))
        def _():
            receive((g - EVENT) // GAP + 1)

        @pl.when(t == 0)
        def _():
            swap_in(zl, 0).wait_recv()

        @pl.when(((t == HEAD) & (k < 3)) | ((t == 0) & (k == 3)))
        def _():
            swap_in(zl, 1).wait_recv()
            swap_in(zl, 2).wait_recv()

        weights(g, False)

        @pl.when(g + NB - 1 < 4 * NT)
        def _():
            weights(g + NB - 1, True)

        @pl.when(g >= 2)
        def _():
            put(g - 2, True)

        b = lax.rem(g, NB)
        o = lax.rem(g, 2)

        def project(rows, outs):
            for r in range(TN // 256):
                cols = slice(r * 256, (r + 1) * 256)
                gate = jnp.dot(rows, wbuf[b, 0, :, cols], preferred_element_type=F32)
                up = jnp.dot(rows, wbuf[b, 1, :, cols], preferred_element_type=F32)
                h = (jax.nn.silu(gate) * up).astype(BF16)
                for m, n in enumerate(outs):
                    hbuf[o, n, :, cols] = h[m * 2 * SLOTS : (m + 1) * 2 * SLOTS, :]

        def held(n):
            return zbuf[pl.ds(pieces[n], 2)].reshape(2 * SLOTS, D)

        @pl.when(pair & jnp.logical_not(lone))
        def _():
            project(jnp.concatenate([held(0), held(1)], axis=0), (0, 1))

        @pl.when(pair & lone)
        def _():
            project(jnp.concatenate([held(0), held(1), held(2)], axis=0), (0, 1, 2))

        @pl.when(lone & (k == 0))
        def _():
            project(held(2), (2,))

        put(g, False)
        return carry

    lax.fori_loop(0, 4 * NT, body, 0)
    put(4 * NT - 2, True)
    put(4 * NT - 1, True)
    for slot in range(4):
        for r in range(3):
            swap(slot, r).wait_send()

        @pl.when((z >= slot) & (z < 3))
        def _():
            for copy in along(x_ref, info_ref, slot, z, 1):
                copy.wait_send()

        @pl.when((z <= slot) & (z > 0))
        def _():
            for copy in along(x_ref, info_ref, slot, z, 0):
                copy.wait_send()

        @pl.when(z != slot)
        def _():
            info_out[slot] = ibuf[slot]

        @pl.when(z == slot)
        def _():
            info_out[slot] = info_ref[...]


W = 256
NS = D // W
KEEP = 6
SKEW = 6
LATE = 5


def down_kernel(info_ref, h_hbm, wd_hbm, y_ref,
                hv, wbuf, obuf, rbuf, stage, ubuf, comb,
                hsem, wsem, osend, orecv, usend, urecv):
    y, z, c = place()
    q = y * 2 + c
    near = z // 2 * 2
    far = 2 - near
    inner = z * (3 - z) // 2
    onward = z + 1 - near
    other = 2 * near + 1 - z
    barrier = pltpu.get_barrier_semaphore()

    def at(zz):
        return {"ep": ep_of(y, zz, c)}

    def peer(r):
        dy, dc = PEERS[r]
        return flip(y, dy), flip(c, dc)

    for r in range(3):
        yy, cc = peer(r)
        pl.semaphore_signal(barrier, inc=1, device_id={"ep": ep_of(yy, z, cc)}, device_id_type=MESH)

    @pl.when(z > 0)
    def _():
        pl.semaphore_signal(barrier, inc=1, device_id=at(z - 1), device_id_type=MESH)

    @pl.when(z < 3)
    def _():
        pl.semaphore_signal(barrier, inc=1, device_id=at(z + 1), device_id_type=MESH)

    def weights(i):
        b = lax.rem(i, 2)
        s = lax.rem(i, NS)
        return pltpu.make_async_copy(
            wd_hbm.at[:, pl.ds(pl.multiple_of(s * W, W), W)], wbuf.at[b], wsem.at[b]
        )

    def h_rows(n):
        rows = pl.ds(pl.multiple_of(n * LAYER, LAYER), LAYER)
        return pltpu.make_async_copy(h_hbm.at[rows], hv.at[rows], hsem.at[n])

    weights(0).start()
    for n in range(2):
        h_rows(far + n).start()
    for d in range(4):
        info = info_ref[d]
        for e in range(4):
            hit = slot_rows(ep_of(e // 2, z, e % 2), info)
            total = jnp.where(hit[0], info[4:5, :], 0.0)
            for j in range(1, 4):
                total += jnp.where(hit[j], info[4 + j : 5 + j, :], 0.0)
            comb[d, e * SLOTS : (e + 1) * SLOTS, :] = total.astype(BF16)
    pl.semaphore_wait(barrier, neighbours(z))

    def across(i, r):
        yy, cc = peer(r)
        half = i // NS
        base = far + half * (near - far)
        s = i - half * NS
        return pltpu.make_async_remote_copy(
            src_ref=obuf.at[lax.rem(i, 2), yy * 2 + cc],
            dst_ref=rbuf.at[s, pl.ds(base, 2), q],
            send_sem=osend.at[lax.rem(i, 2), r],
            recv_sem=orecv.at[s, q, half],
            device_id={"ep": ep_of(yy, z, cc)},
            device_id_type=MESH,
        )

    def across_in(s, r, half):
        yy, cc = peer(r)
        base = near if half else far
        return pltpu.make_async_remote_copy(
            src_ref=obuf.at[0, 0],
            dst_ref=rbuf.at[s, pl.ds(base, 2), yy * 2 + cc],
            send_sem=osend.at[0, r],
            recv_sem=orecv.at[s, yy * 2 + cc, half],
            device_id={"ep": ep_of(yy, z, cc)},
            device_id_type=MESH,
        )

    def hop(s, n, to, slot):
        return pltpu.make_async_remote_copy(
            src_ref=stage.at[lax.rem(s, KEEP), n],
            dst_ref=ubuf.at[s, slot],
            send_sem=usend.at[lax.rem(s, KEEP), n],
            recv_sem=urecv.at[s, slot],
            device_id=at(to),
            device_id_type=MESH,
        )

    def far_hop(s, n):
        last = z // 2 * (3 - z) * n
        d = far + n
        return hop(s, n, onward, d + last * (4 - d))

    def near_hop(s):
        return hop(s, 2, other, other + lax.rem(z, 2) * (4 - other))

    def arrived(s, slot):
        hop(s, 2, z, slot).wait_recv()

    def live(s):
        return (s >= 0) & (s < NS)

    def clamp(s):
        w = (s + 2 * NS) // NS
        inside = (w - 1) * (3 - w)
        return inside * s + (1 - inside) * NS, inside

    def part(s, d):
        rows = rbuf[s, d].reshape(LAYER, W)
        return lax.dot_general(comb[d], rows, (((0,), (0,)), ((), ())), preferred_element_type=F32)

    def far_part(s):
        at_s, inside = clamp(s)
        slot = inside * lax.rem(s + 2 * KEEP, KEEP) + (1 - inside) * KEEP
        for n in range(2):
            came = jnp.where(inner == 1, ubuf[at_s, far + n].astype(F32), 0.0)
            stage[slot, n] = (part(at_s, far + n) + came).astype(BF16)

    def near_part(s):
        at_s, inside = clamp(s)
        slot = inside * lax.rem(s + 2 * KEEP, KEEP) + (1 - inside) * KEEP
        came = jnp.where(inner == 1, ubuf[at_s, other].astype(F32), 0.0)
        stage[slot, 2] = (part(at_s, other) + came).astype(BF16)

    def finish(s):
        at_s, inside = clamp(s)
        below = jnp.where(z > 0, ubuf[at_s, z].astype(F32), 0.0)
        above = jnp.where(z < 3, ubuf[at_s, 4].astype(F32), 0.0)
        total = part(at_s, z) + below + above
        y_ref[:, pl.ds(pl.multiple_of(inside * s * W, W), W)] = total.astype(BF16)

    def body(i, carry):
        s_far = i - 2 - SKEW * inner
        s_near = i - NS - 2
        s_out = s_near - LATE

        def wait_out():
            @pl.when(live(s_out))
            def _():
                @pl.when(z > 0)
                def _():
                    arrived(s_out, z)

                @pl.when(z < 3)
                def _():
                    arrived(s_out, 4)

        @pl.when(live(s_far))
        def _():
            for r in range(3):
                across_in(s_far, r, 0).wait_recv()
            for n in range(2):
                @pl.when(inner == 1)
                def _(n=n):
                    arrived(s_far, far + n)

                @pl.when(s_far >= KEEP)
                def _(n=n):
                    far_hop(s_far - KEEP, n).wait_send()

        @pl.when(live(s_near))
        def _():
            for r in range(3):
                across_in(s_near, r, 1).wait_recv()

            @pl.when(inner == 1)
            def _():
                arrived(s_near, other)

            @pl.when(s_near >= KEEP)
            def _():
                near_hop(s_near - KEEP).wait_send()

        @pl.when(i < 2 * NS)
        def _():
            wait_out()
            b = lax.rem(i, 2)
            weights(i).wait()

            @pl.when(i + 1 < 2 * NS)
            def _():
                weights(i + 1).start()

            @pl.when(i >= 2)
            def _():
                for r in range(3):
                    across(i - 2, r).wait_send()

            @pl.when(i == 0)
            def _():
                for n in range(2):
                    h_rows(far + n).wait()
                for n in range(2):
                    h_rows(near + n).start()

            @pl.when(i == NS)
            def _():
                for n in range(2):
                    h_rows(near + n).wait()

            def rows(base):
                out = jnp.dot(
                    hv[pl.ds(pl.multiple_of(base * LAYER, 2 * LAYER), 2 * LAYER), :],
                    wbuf[b],
                    preferred_element_type=F32,
                ).astype(BF16)
                for m in range(8):
                    obuf[b, m % 4, m // 4] = out[m * SLOTS : (m + 1) * SLOTS, :]
                far_part(s_far)

            @pl.when(i < NS)
            def _():
                rows(far)
                rbuf[i, pl.ds(far, 2), q] = obuf[b, q]

            @pl.when(i >= NS)
            def _():
                rows(near)
                near_part(s_near)
                finish(s_out)
                rbuf[i - NS, pl.ds(near, 2), q] = obuf[b, q]

            for r in (1, 2, 0):
                across(i, r).start()

        @pl.when(live(s_far))
        def _():
            for n in (1, 0):
                far_hop(s_far, n).start()

        @pl.when((i >= 2 * NS) & live(s_near))
        def _():
            near_part(s_near)

        @pl.when(live(s_near))
        def _():
            near_hop(s_near).start()

        @pl.when((i >= 2 * NS) & live(s_out))
        def _():
            wait_out()
            finish(s_out)

        return carry

    lax.fori_loop(0, 2 * NS + 2 + LATE, body, 0)
    for i in (2 * NS - 2, 2 * NS - 1):
        for r in range(3):
            across(i, r).wait_send()
    for s in range(NS - KEEP, NS):
        for n in range(2):
            far_hop(s, n).wait_send()
        near_hop(s).wait_send()


def any_space():
    return pl.BlockSpec(memory_space=pl.ANY)


def vmem():
    return pl.BlockSpec(memory_space=pltpu.VMEM)


def project_up(info, x, wg, wu):
    rows = 16 * SLOTS
    return pl.pallas_call(
        up_kernel,
        out_shape=(jax.ShapeDtypeStruct((rows, FF), BF16), jax.ShapeDtypeStruct((4, 8, TOK), F32)),
        in_specs=[vmem(), vmem(), any_space(), any_space()],
        out_specs=(any_space(), vmem()),
        scratch_shapes=[
            pltpu.VMEM((4, TOK, D), BF16),
            pltpu.VMEM((16, SLOTS, D), BF16),
            pltpu.VMEM((4, 3, SLOTS, D), BF16),
            pltpu.VMEM((4, 8, TOK), F32),
            pltpu.VMEM((NB, 2, D, TN), BF16),
            pltpu.VMEM((2, 3, 2 * SLOTS, TN), BF16),
            pltpu.SemaphoreType.DMA((NB, 2, KSPLIT)),
            pltpu.SemaphoreType.DMA((2, 3)),
            pltpu.SemaphoreType.DMA((4, 3)),
            pltpu.SemaphoreType.DMA((16,)),
            pltpu.SemaphoreType.DMA((2, 4)),
            pltpu.SemaphoreType.DMA((4,)),
            pltpu.SemaphoreType.DMA((2, 4)),
            pltpu.SemaphoreType.DMA((4,)),
        ],
        compiler_params=pltpu.CompilerParams(
            collective_id=0, has_side_effects=True, vmem_limit_bytes=VMEM_LIMIT
        ),
        cost_estimate=pl.CostEstimate(
            flops=4 * rows * D * FF, bytes_accessed=16 * D * FF + 2 * rows * FF, transcendentals=rows * FF
        ),
        name="project_up",
    )(info, x, wg, wu)


def project_down(info, h, wd):
    rows = 16 * SLOTS
    return pl.pallas_call(
        down_kernel,
        out_shape=jax.ShapeDtypeStruct((TOK, D), BF16),
        in_specs=[vmem(), any_space(), any_space()],
        out_specs=vmem(),
        scratch_shapes=[
            pltpu.VMEM((rows, FF), BF16),
            pltpu.VMEM((2, FF, W), BF16),
            pltpu.VMEM((2, 4, 2, SLOTS, W), BF16),
            pltpu.VMEM((NS + 1, 4, 4, SLOTS, W), BF16),
            pltpu.VMEM((KEEP + 1, 3, TOK, W), BF16),
            pltpu.VMEM((NS + 1, 5, TOK, W), BF16),
            pltpu.VMEM((4, LAYER, TOK), BF16),
            pltpu.SemaphoreType.DMA((4,)),
            pltpu.SemaphoreType.DMA((2,)),
            pltpu.SemaphoreType.DMA((2, 3)),
            pltpu.SemaphoreType.DMA((NS, 4, 2)),
            pltpu.SemaphoreType.DMA((KEEP, 3)),
            pltpu.SemaphoreType.DMA((NS, 5)),
        ],
        compiler_params=pltpu.CompilerParams(
            collective_id=1, has_side_effects=True, vmem_limit_bytes=VMEM_LIMIT
        ),
        cost_estimate=pl.CostEstimate(
            flops=2 * rows * D * FF, bytes_accessed=2 * D * FF + 2 * rows * FF, transcendentals=0
        ),
        name="project_down",
    )(info, h, wd)


def solution(mesh):
    def step(x, expert, slot, gate, wg, wu, wd):
        where = jnp.where(slot[0, 0] < SLOTS, expert[0, 0] * SLOTS + slot[0, 0], -1).astype(F32)
        info = jnp.concatenate([where.T, gate[0, 0].T], axis=0)
        h, infos = project_up(info, x[0, 0], wg[0], wu[0])
        return project_down(infos, h, wd[0])[None, None]

    tokens = P("dp", "ep")
    experts = P("ep")
    return jax.shard_map(
        step,
        mesh=mesh,
        in_specs=(tokens, tokens, tokens, tokens, experts, experts, experts),
        out_specs=tokens,
        check_vma=False,
    )
```
